256 devices in a mesh: dp: 8 (over x, z_lo), seq: 32 (over y, z_hi, core).
Axes of the slice: x: 4, y: 4, z: 8 (z_hi: 4, z_lo: 2; z = z_hi * 2 + z_lo), core: 2. Of those that a mesh axis runs over, the one named last changes fastest.
Arguments:
- query: bfloat16 [4096, 3072], P('seq', 'dp'), may hold values from -300 to 300
- key: bfloat16 [4096, 3072], P('seq', 'dp'), may hold values from -10 to 10
- value: bfloat16 [4096, 3072], P('seq', 'dp'), may hold values from -6 to 6
- d_query: bfloat16 [4096, 3072], P('seq', 'dp'), may hold values from -6 to 6
- d_key: bfloat16 [4096, 3072], P('seq', 'dp'), may hold values from -6 to 6
- d_value: bfloat16 [4096, 3072], P('seq', 'dp'), may hold values from -6 to 6
- residual: bfloat16 [4096, 3072], P('seq', 'dp'), may hold values from -6 to 6
- d_residual: bfloat16 [4096, 3072], P('seq', 'dp'), may hold values from -6 to 6
- w_in: bfloat16 [3072, 7168], P('seq', 'dp'), may hold values from -0.109375 to 0.109375
- w_out: bfloat16 [7168, 3072], P(('dp', 'seq')), may hold values from -0.3125 to 0.3125
Outputs:
- block_out: bfloat16 [4096, 3072], P('seq', 'dp')
- d_block_out: bfloat16 [4096, 3072], P('seq', 'dp')
The draws below stay inside these ranges and needn't reach their ends.
All inputs are finite; a program needn't handle non-finite values.
Results may differ from the reference program's by a relative error of at most 0.025.
Values may be sent and summed in bfloat16 or wider, within the bound.
No kernel may reach another device: no remote copies, remote signals or barrier semaphores. Data moves between devices by JAX's collectives and lax.ppermute only.
A program may use at most 128 MiB of HBM per device.

```python
import jax
import jax.numpy as jnp
from jax import lax

HEAD_DIM = 128
HEADS = 24
D = 3072
FF = 7168
LENGTH = 4096


def joint_draw(base_key):
    folded = jax.random.fold_in(base_key, 11)
    key_a, key_b = jax.random.split(folded, 2)
    keys_arr = jnp.clip(jax.random.normal(key_a, (LENGTH, D), jnp.float32), -5.0, 5.0)
    queries = jnp.clip(jax.random.normal(key_b, (LENGTH, D), jnp.float32), -5.0, 5.0)
    return (queries, keys_arr)


def draw_query(base_key, part):
    return joint_draw(base_key)[0].astype(jnp.bfloat16)


def draw_key(base_key, part):
    return joint_draw(base_key)[1].astype(jnp.bfloat16)


def raised(values, key, source, target, parts, factor):
    owner, partner = [(jnp.arange(values.shape[position]) // (values.shape[position] // parts)).reshape([-1 if axis == position else 1 for axis in range(values.ndim)]) for position in (source, target)]
    chosen = jax.random.permutation(key, parts)[partner]
    strong = (owner == chosen) | (owner == (partner + parts // 2) % parts)
    return jnp.where(strong, factor * values, values)


def shard_levels(rng, shape, cuts, low, top_value):
    loudness = 1.0
    for position, blocks in cuts:
        draws = jax.random.uniform(jax.random.fold_in(jax.random.fold_in(rng, 6), position), (blocks,), jnp.float32, low / len(cuts), top_value / len(cuts))
        loudness = loudness * jnp.repeat(jnp.exp(draws), shape[position] // blocks).reshape((-1,) + (1,) * (len(shape) - 1 - position))
    return loudness


def scatter_about(rng, shape, deviation, bound, pieces=(), dtype=jnp.bfloat16):
    entries = deviation * jax.random.normal(rng, shape, jnp.float32)
    if pieces:
        entries = entries * shard_levels(rng, shape, pieces, -0.22, 0.18)
    return jnp.clip(entries, -bound, bound).astype(dtype)


def heavy_noise(rng, extent, spread, bound, pieces, heavy, held_as=jnp.bfloat16):
    result = spread * jax.random.normal(rng, extent, jnp.float32)
    if pieces:
        result = result * shard_levels(rng, extent, pieces, -0.22, 0.18)
    return jnp.clip(raised(result, jax.random.fold_in(rng, 3), *heavy), -bound, bound).astype(held_as)


def setup_inputs(seed: int = 0) -> dict:
    keys = jax.random.split(jax.random.key(seed), 11)
    query = draw_query(jax.random.fold_in(keys[10], 71), 0)
    key = draw_key(jax.random.fold_in(keys[10], 71), 0)
    value = scatter_about(keys[2], (LENGTH, D), 1.0, 6.0, ((0, 32), (1, 8)))
    d_query = scatter_about(keys[3], (LENGTH, D), 1.0, 6.0, ((0, 32), (1, 8)))
    d_key = scatter_about(keys[4], (LENGTH, D), 1.0, 6.0, ((0, 32), (1, 8)))
    d_value = scatter_about(keys[5], (LENGTH, D), 1.0, 6.0, ((0, 32), (1, 8)))
    residual = scatter_about(keys[6], (LENGTH, D), 1.0, 6.0, ((0, 32), (1, 8)))
    d_residual = scatter_about(keys[7], (LENGTH, D), 1.0, 6.0, ((0, 32), (1, 8)))
    w_in = scatter_about(keys[8], (D, FF), D ** -0.5, 0.109375, ((0, 32), (1, 8)))
    w_out = heavy_noise(keys[9], (FF, D), FF ** -0.5, 0.3125, ((0, 256),), (0, 1, 256, 6.0))
    return dict(query=query, key=key, value=value, d_query=d_query, d_key=d_key, d_value=d_value, residual=residual, d_residual=d_residual, w_in=w_in, w_out=w_out)


gelu_coeff = 0.7978845608
cubic_coeff = 0.044715

def gelu_pair(pre_act, d_pre_act):
    inner_arg = gelu_coeff * (pre_act + cubic_coeff * pre_act * pre_act * pre_act)
    hyper = jnp.tanh(inner_arg)
    gelu_value = 0.5 * pre_act * (1.0 + hyper)
    gelu_slope = 0.5 * (1.0 + hyper) + 0.5 * pre_act * (1.0 - hyper * hyper) * gelu_coeff * (1.0 + 3.0 * cubic_coeff * pre_act * pre_act)
    return (gelu_value, gelu_slope * d_pre_act)

def head_attend(operands):
    query_head, key_head, value_head, dquery_head, dkey_head, dvalue_head = operands
    score_scale = 1.0 / jnp.sqrt(jnp.float32(HEAD_DIM))
    scores = jnp.dot(query_head, key_head.T, preferred_element_type=jnp.float32) * score_scale
    d_scores = (jnp.dot(dquery_head, key_head.T, preferred_element_type=jnp.float32) + jnp.dot(query_head, dkey_head.T, preferred_element_type=jnp.float32)) * score_scale
    row_peak = lax.optimization_barrier(jnp.max(scores, axis=1, keepdims=True))
    weights = jnp.exp(scores - row_peak)
    row_total = lax.optimization_barrier(jnp.sum(weights, axis=1))
    mixed = weights * d_scores
    row_slope = lax.optimization_barrier(jnp.sum(mixed, axis=1))
    weights_low = weights.astype(jnp.bfloat16)
    mixed_low = mixed.astype(jnp.bfloat16)
    accum = jnp.dot(weights_low, value_head, preferred_element_type=jnp.float32)
    tangent = jnp.dot(mixed_low, value_head, preferred_element_type=jnp.float32) + jnp.dot(weights_low, dvalue_head, preferred_element_type=jnp.float32)
    attended = accum / row_total[:, None]
    d_attended = tangent / row_total[:, None] - (row_slope / row_total)[:, None] * attended
    return (attended, d_attended)

def split_heads(array):
    return array.reshape(LENGTH, HEADS, HEAD_DIM).transpose(1, 0, 2)

def reference(query, key, value, d_query, d_key, d_value, residual, d_residual, w_in, w_out):
    operands = tuple((split_heads(array) for array in (query, key, value, d_query, d_key, d_value)))
    attended, d_attended = lax.map(head_attend, operands)
    attended = attended.transpose(1, 0, 2).reshape(LENGTH, D)
    d_attended = d_attended.transpose(1, 0, 2).reshape(LENGTH, D)
    mixed_in = (residual.astype(jnp.float32) + attended).astype(jnp.bfloat16)
    d_mixed_in = (d_residual.astype(jnp.float32) + d_attended).astype(jnp.bfloat16)
    pre_act = jnp.dot(mixed_in, w_in, preferred_element_type=jnp.float32)
    d_pre_act = jnp.dot(d_mixed_in, w_in, preferred_element_type=jnp.float32)
    hidden, d_hidden = gelu_pair(pre_act, d_pre_act)
    hidden = hidden.astype(jnp.bfloat16)
    d_hidden = d_hidden.astype(jnp.bfloat16)
    block_out = (mixed_in.astype(jnp.float32) + jnp.dot(hidden, w_out, preferred_element_type=jnp.float32)).astype(jnp.bfloat16)
    d_block_out = (d_mixed_in.astype(jnp.float32) + jnp.dot(d_hidden, w_out, preferred_element_type=jnp.float32)).astype(jnp.bfloat16)
    return (block_out, d_block_out)
```

```python
import functools
import math

import jax
import jax.numpy as jnp
from jax import lax
from jax.experimental import pallas as pl
from jax.experimental.pallas import tpu as pltpu
from jax.sharding import Mesh, PartitionSpec as P

HEAD_DIM = 128

gelu_coeff = 0.7978845608
cubic_coeff = 0.044715

NX, NL, NY, NH = 4, 2, 4, 4
STAT_ROWS = 16


def gelu_pair(pre_act, d_pre_act):
    inner_arg = gelu_coeff * (pre_act + cubic_coeff * pre_act * pre_act * pre_act)
    hyper = jnp.tanh(inner_arg)
    gelu_value = 0.5 * pre_act * (1.0 + hyper)
    gelu_slope = 0.5 * (1.0 + hyper) + 0.5 * pre_act * (1.0 - hyper * hyper) * gelu_coeff * (
        1.0 + 3.0 * cubic_coeff * pre_act * pre_act
    )
    return (gelu_value, gelu_slope * d_pre_act)


def shift(value, axis, step):
    size = lax.axis_size(axis)
    return lax.ppermute(value, axis, [(i, (i + step) % size) for i in range(size)])


def shift_dp(value, dx, dz):
    pairs = [
        (i * NL + j, ((i + dx) % NX) * NL + (j + dz) % NL) for i in range(NX) for j in range(NL)
    ]
    return lax.ppermute(value, ("x", "zl"), pairs)


DP_STEPS = [(dx, dz) for dx in range(NX) for dz in range(NL)]


def split3(value):
    high = value.astype(jnp.bfloat16).astype(jnp.float32)
    rest = value - high
    middle = rest.astype(jnp.bfloat16).astype(jnp.float32)
    return high, middle, rest - middle


def attend_kernel(*refs):
    q_refs, kv_refs, out_refs = refs[:4], refs[4:12], refs[12:16]
    rows = q_refs[0].shape[1]
    scale = 1.0 / math.sqrt(HEAD_DIM)
    nt = (((1,), (1,)), ((), ()))
    for h in range(q_refs[0].shape[2] // HEAD_DIM):
        at = slice(h * HEAD_DIM, (h + 1) * HEAD_DIM)
        k, v, dk, dv = (
            jnp.concatenate([ref[j, :, at] for ref in kv_refs], axis=0) for j in range(4)
        )
        k_dk = jnp.concatenate([k, dk], axis=1)
        v_dv = jnp.concatenate([v, dv], axis=1)
        for pair in range(2):
            ours = q_refs[2 * pair : 2 * pair + 2]
            q = jnp.concatenate([ref[0, :, at] for ref in ours], axis=0)
            dq = jnp.concatenate([ref[1, :, at] for ref in ours], axis=0)
            scores = lax.dot_general(q, k, nt, preferred_element_type=jnp.float32) * scale
            d_scores = lax.dot_general(
                jnp.concatenate([dq, q], axis=1), k_dk, nt, preferred_element_type=jnp.float32
            )
            d_scores = d_scores * scale
            peak = jnp.max(scores, axis=1, keepdims=True)
            weights = jnp.exp(scores - peak)
            mixed = weights * d_scores
            total = jnp.sum(weights, axis=1, keepdims=True)
            slope = jnp.sum(mixed, axis=1, keepdims=True)
            both = jnp.dot(weights.astype(jnp.bfloat16), v_dv, preferred_element_type=jnp.float32)
            tangent = both[:, HEAD_DIM:] + jnp.dot(
                mixed.astype(jnp.bfloat16), v, preferred_element_type=jnp.float32
            )
            share = 1.0 / total
            sigma = slope * share
            attended = both[:, :HEAD_DIM] * share
            d_attended = tangent * share - sigma * attended
            parts = split3(peak + jnp.log(total)) + split3(sigma)
            lane = lax.broadcasted_iota(jnp.int32, (2 * rows, HEAD_DIM), 1)
            table = jnp.zeros((2 * rows, HEAD_DIM), jnp.float32)
            for n, part in enumerate(parts):
                table = jnp.where(lane == n, part, table)
            for b in range(2):
                mine = slice(b * rows, (b + 1) * rows)
                out = out_refs[2 * pair + b]
                out[0:rows, at] = attended[mine].astype(jnp.bfloat16)
                out[rows : 2 * rows, at] = d_attended[mine].astype(jnp.bfloat16)
                out[2 * rows : 2 * rows + STAT_ROWS, at] = table[mine].T[:STAT_ROWS].astype(
                    jnp.bfloat16
                )


def combine_kernel(*refs):
    part_refs, res_ref, dres_ref, out_ref = refs[:4], refs[4], refs[5], refs[6]
    rows = res_ref.shape[0]
    for h in range(res_ref.shape[1] // HEAD_DIM):
        at = slice(h * HEAD_DIM, (h + 1) * HEAD_DIM)
        logs, sigmas = [], []
        for ref in part_refs:
            table = ref[2 * rows : 2 * rows + STAT_ROWS, at].astype(jnp.float32)
            table = jnp.concatenate(
                [table, jnp.zeros((HEAD_DIM - STAT_ROWS, rows), jnp.float32)], axis=0
            ).T
            logs.append(table[:, 0:1] + table[:, 1:2] + table[:, 2:3])
            sigmas.append(table[:, 3:4] + table[:, 4:5] + table[:, 5:6])
        peak = functools.reduce(jnp.maximum, logs)
        shares = [jnp.exp(log - peak) for log in logs]
        norm = 1.0 / sum(shares)
        shares = [share * norm for share in shares]
        sigma = sum(p * s for p, s in zip(shares, sigmas))
        attended = jnp.zeros((rows, HEAD_DIM), jnp.float32)
        d_attended = jnp.zeros((rows, HEAD_DIM), jnp.float32)
        for ref, p, s in zip(part_refs, shares, sigmas):
            a = ref[0:rows, at].astype(jnp.float32)
            d = ref[rows : 2 * rows, at].astype(jnp.float32)
            attended = attended + p * a
            d_attended = d_attended + p * (d + (s - sigma) * a)
        mixed = res_ref[:, at].astype(jnp.float32) + attended
        d_mixed = dres_ref[:, at].astype(jnp.float32) + d_attended
        out_ref[0:rows, at] = mixed.astype(jnp.bfloat16)
        out_ref[rows : 2 * rows, at] = d_mixed.astype(jnp.bfloat16)


def feed_kernel(place_ref, *refs):
    x_refs, w_in_ref, w_out_refs, out_refs = refs[:8], refs[8], refs[9:11], refs[11:19]
    two_rows, width = x_refs[0].shape
    rows = two_rows // 2
    half = w_out_refs[0].shape[1]
    pre = jnp.zeros((two_rows, w_in_ref.shape[1]), jnp.float32)
    for n in range(8):
        at = pl.multiple_of(place_ref[n] * width, width)
        pre = pre + jnp.dot(
            x_refs[n][...], w_in_ref[pl.ds(at, width), :], preferred_element_type=jnp.float32
        )
    hidden, d_hidden = gelu_pair(pre[:rows], pre[rows:])
    hidden = jnp.concatenate([hidden.astype(jnp.bfloat16), d_hidden.astype(jnp.bfloat16)], axis=0)
    for n in range(8):
        place = place_ref[8 + n]

        for side in range(2):

            @pl.when(place // (half // width) == side)
            def _():
                at = pl.multiple_of((place % (half // width)) * width, width)
                out = jnp.dot(
                    hidden,
                    w_out_refs[side][:, pl.ds(at, width)],
                    preferred_element_type=jnp.float32,
                )
                out_refs[n][...] = out.astype(jnp.bfloat16)


def whole():
    return pl.BlockSpec(memory_space=pltpu.VMEM)


def on_device(query, key, value, d_query, d_key, d_value, residual, d_residual, w_in, w_out):
    rows, width = query.shape
    core = lax.axis_index("c")
    bf16 = jnp.bfloat16

    w_out_twin = shift(w_out, "c", 1)
    w_out_low = jnp.where(core == 0, w_out, w_out_twin)
    w_out_high = jnp.where(core == 0, w_out_twin, w_out)
    half = w_out.shape[1] // 2
    w_out_pair = jnp.concatenate([w_out_low, w_out_high], axis=0)
    w_out_mine = lax.dynamic_slice_in_dim(w_out_pair, core * half, half, 1)
    w_in_whole = lax.all_gather(w_in, ("y", "zh", "c"), axis=0, tiled=True)
    w_out_half = lax.all_gather(w_out_mine, ("y", "zh"), axis=0, tiled=True)
    w_out_other = shift(w_out_half, "c", 1)
    w_out_left = jnp.where(core == 0, w_out_half, w_out_other)
    w_out_right = jnp.where(core == 0, w_out_other, w_out_half)

    kv = jnp.stack([key, value, d_key, d_value])
    qs = jnp.stack([query, d_query])
    steps = (1, -1, 2)
    q_pieces = [qs] + [shift(qs, "zh", s) for s in steps]
    kv_pieces = [kv] + [shift(kv, "y", s) for s in steps]
    kv_pieces = kv_pieces + [shift(piece, "c", 1) for piece in kv_pieces]
    message = jax.ShapeDtypeStruct((2 * rows + STAT_ROWS, width), bf16)
    parts = pl.pallas_call(
        attend_kernel,
        out_shape=[message] * 4,
        in_specs=[whole()] * 12,
        out_specs=[whole()] * 4,
        compiler_params=pltpu.CompilerParams(vmem_limit_bytes=48 << 20),
        cost_estimate=pl.CostEstimate(
            flops=2_415_919_104, bytes_accessed=6_000_000, transcendentals=1_572_864
        ),
        name="attend",
    )(*q_pieces, *kv_pieces)
    parts = [parts[0]] + [shift(part, "zh", -s) for part, s in zip(parts[1:], steps)]
    x = pl.pallas_call(
        combine_kernel,
        out_shape=jax.ShapeDtypeStruct((2 * rows, width), bf16),
        in_specs=[whole()] * 6,
        out_specs=whole(),
        cost_estimate=pl.CostEstimate(
            flops=2_000_000, bytes_accessed=1_300_000, transcendentals=2_000
        ),
        name="combine",
    )(*parts, residual, d_residual)

    px, pz = lax.axis_index("x"), lax.axis_index("zl")
    place = jnp.stack(
        [((px - dx) % NX) * NL + (pz - dz) % NL for dx, dz in DP_STEPS]
        + [((px + dx) % NX) * NL + (pz + dz) % NL for dx, dz in DP_STEPS]
    ).astype(jnp.int32)
    xs = [x] + [shift_dp(x, dx, dz) for dx, dz in DP_STEPS[1:]]
    sums = pl.pallas_call(
        feed_kernel,
        out_shape=[jax.ShapeDtypeStruct((2 * rows, width), bf16)] * 8,
        in_specs=[pl.BlockSpec(memory_space=pltpu.SMEM)] + [whole()] * 11,
        out_specs=[whole()] * 8,
        compiler_params=pltpu.CompilerParams(vmem_limit_bytes=48 << 20),
        cost_estimate=pl.CostEstimate(
            flops=2_818_572_288, bytes_accessed=14_000_000, transcendentals=120_000
        ),
        name="feed",
    )(place, *xs, w_in_whole, w_out_left, w_out_right)
    sums = [sums[0]] + [shift_dp(s, dx, dz) for s, (dx, dz) in zip(sums[1:], DP_STEPS[1:])]
    total = x.astype(jnp.float32)
    for s in sums:
        total = total + s.astype(jnp.float32)
    total = total.astype(bf16)
    return (total[:rows], total[rows:])


def solution(mesh):
    fine = Mesh(mesh.devices.reshape(NX, NL, NY, NH, 2), ("x", "zl", "y", "zh", "c"))
    dp, seq = ("x", "zl"), ("y", "zh", "c")
    tokens = P(seq, dp)
    return jax.shard_map(
        on_device,
        mesh=fine,
        in_specs=(tokens,) * 9 + (P(dp + seq, None),),
        out_specs=(tokens, tokens),
        check_vma=False,
    )
```

```python
import functools
import math

import jax
import jax.numpy as jnp
from jax import lax
from jax.experimental import pallas as pl
from jax.experimental.pallas import tpu as pltpu
from jax.sharding import Mesh, PartitionSpec as P

HEAD_DIM = 128

gelu_coeff = 0.7978845608
cubic_coeff = 0.044715

NX, NL, NY, NH = 4, 2, 4, 4
STAT_ROWS = 8


def gelu_pair(pre_act, d_pre_act):
    inner_arg = gelu_coeff * (pre_act + cubic_coeff * pre_act * pre_act * pre_act)
    hyper = jnp.tanh(inner_arg)
    gelu_value = 0.5 * pre_act * (1.0 + hyper)
    gelu_slope = 0.5 * (1.0 + hyper) + 0.5 * pre_act * (1.0 - hyper * hyper) * gelu_coeff * (
        1.0 + 3.0 * cubic_coeff * pre_act * pre_act
    )
    return (gelu_value, gelu_slope * d_pre_act)


def shift(value, axis, step):
    size = lax.axis_size(axis)
    return lax.ppermute(value, axis, [(i, (i + step) % size) for i in range(size)])


def shift_dp(value, dx, dz):
    pairs = [
        (i * NL + j, ((i + dx) % NX) * NL + (j + dz) % NL) for i in range(NX) for j in range(NL)
    ]
    return lax.ppermute(value, ("x", "zl"), pairs)


DP_STEPS = [(dx, dz) for dx in range(NX) for dz in range(NL)]


def split3(value):
    high = value.astype(jnp.bfloat16).astype(jnp.float32)
    rest = value - high
    middle = rest.astype(jnp.bfloat16).astype(jnp.float32)
    return high, middle, rest - middle


def attend_kernel(*refs):
    q_refs, kv_refs, out_refs = refs[:4], refs[4:12], refs[12:16]
    rows = q_refs[0].shape[1]
    scale = 1.0 / math.sqrt(HEAD_DIM)
    nt = (((1,), (1,)), ((), ()))
    for h in range(q_refs[0].shape[2] // HEAD_DIM):
        at = slice(h * HEAD_DIM, (h + 1) * HEAD_DIM)
        k, v, dk, dv = (
            jnp.concatenate([ref[j, :, at] for ref in kv_refs], axis=0) for j in range(4)
        )
        k_dk = jnp.concatenate([k, dk], axis=1)
        v_dv = jnp.concatenate([v, dv], axis=1)
        for pair in range(2):
            ours = q_refs[2 * pair : 2 * pair + 2]
            q = jnp.concatenate([ref[0, :, at] for ref in ours], axis=0)
            dq = jnp.concatenate([ref[1, :, at] for ref in ours], axis=0)
            scores = lax.dot_general(q, k, nt, preferred_element_type=jnp.float32) * scale
            d_scores = lax.dot_general(
                jnp.concatenate([dq, q], axis=1), k_dk, nt, preferred_element_type=jnp.float32
            )
            d_scores = d_scores * scale
            peak = jnp.max(scores, axis=1, keepdims=True)
            weights = jnp.exp(scores - peak)
            mixed = weights * d_scores
            total = jnp.sum(weights, axis=1, keepdims=True)
            slope = jnp.sum(mixed, axis=1, keepdims=True)
            both = jnp.dot(weights.astype(jnp.bfloat16), v_dv, preferred_element_type=jnp.float32)
            tangent = both[:, HEAD_DIM:] + jnp.dot(
                mixed.astype(jnp.bfloat16), v, preferred_element_type=jnp.float32
            )
            share = 1.0 / total
            sigma = slope * share
            attended = both[:, :HEAD_DIM] * share
            d_attended = tangent * share - sigma * attended
            parts = split3(peak + jnp.log(total)) + split3(sigma)
            lane = lax.broadcasted_iota(jnp.int32, (2 * rows, HEAD_DIM), 1)
            table = jnp.zeros((2 * rows, HEAD_DIM), jnp.float32)
            for n, part in enumerate(parts):
                table = jnp.where(lane == n, part, table)
            for b in range(2):
                mine = slice(b * rows, (b + 1) * rows)
                out = out_refs[2 * pair + b]
                out[0:rows, at] = attended[mine].astype(jnp.bfloat16)
                out[rows : 2 * rows, at] = d_attended[mine].astype(jnp.bfloat16)
                out[2 * rows : 2 * rows + STAT_ROWS, at] = table[mine].T[:STAT_ROWS].astype(
                    jnp.bfloat16
                )


def combine_kernel(*refs):
    part_refs, res_ref, dres_ref, out_ref = refs[:4], refs[4], refs[5], refs[6]
    rows = res_ref.shape[0]
    heads = res_ref.shape[1] // HEAD_DIM
    table = []
    for h in range(heads):
        at = slice(h * HEAD_DIM, (h + 1) * HEAD_DIM)
        stats = [ref[2 * rows : 2 * rows + STAT_ROWS, at].astype(jnp.float32) for ref in part_refs]
        logs = [s[0:1] + s[1:2] + s[2:3] for s in stats]
        sigmas = [s[3:4] + s[4:5] + s[5:6] for s in stats]
        peak = functools.reduce(jnp.maximum, logs)
        shares = [jnp.exp(log - peak) for log in logs]
        norm = 1.0 / sum(shares)
        shares = [share * norm for share in shares]
        sigma = sum(p * s for p, s in zip(shares, sigmas))
        table += shares + [p * (s - sigma) for p, s in zip(shares, sigmas)]
    table.append(jnp.zeros((HEAD_DIM - 8 * heads, rows), jnp.float32))
    table = jnp.concatenate(table, axis=0).T
    for h in range(heads):
        at = slice(h * HEAD_DIM, (h + 1) * HEAD_DIM)
        attended = jnp.zeros((rows, HEAD_DIM), jnp.float32)
        d_attended = jnp.zeros((rows, HEAD_DIM), jnp.float32)
        for n, ref in enumerate(part_refs):
            a = ref[0:rows, at].astype(jnp.float32)
            d = ref[rows : 2 * rows, at].astype(jnp.float32)
            p = table[:, 8 * h + n : 8 * h + n + 1]
            r = table[:, 8 * h + 4 + n : 8 * h + 5 + n]
            attended = attended + p * a
            d_attended = d_attended + (p * d + r * a)
        mixed = res_ref[:, at].astype(jnp.float32) + attended
        d_mixed = dres_ref[:, at].astype(jnp.float32) + d_attended
        out_ref[0:rows, at] = mixed.astype(jnp.bfloat16)
        out_ref[rows : 2 * rows, at] = d_mixed.astype(jnp.bfloat16)


def pack_kernel(core_ref, w_in_ref, w_out_ref, twin_ref, out_ref):
    own, width = w_in_ref.shape
    few, half = w_out_ref.shape[0], w_out_ref.shape[1] // 2
    lanes = HEAD_DIM
    for j in range(width // lanes):
        out_ref[j * own : (j + 1) * own] = w_in_ref[:, j * lanes : (j + 1) * lanes]
    base = own * (width // lanes)
    for core in range(2):

        @pl.when(core_ref[0] == core)
        def _():
            pair = (w_out_ref, twin_ref) if core == 0 else (twin_ref, w_out_ref)
            for j in range(half // lanes):
                at = slice(core * half + j * lanes, core * half + (j + 1) * lanes)
                block = jnp.concatenate([ref[:, at].astype(jnp.float32) for ref in pair], axis=0)
                start = base + j * 2 * few
                out_ref[start : start + 2 * few] = block.astype(jnp.bfloat16)


def feed_kernel(parts, place_ref, *refs):
    n_views = 1 + max(view for view, *_ in parts)
    x_refs, w_refs, refs = refs[:8], refs[8 : 8 + n_views], refs[8 + n_views :]
    out_refs, (w_in_ref, w_out_ref, sems) = refs[:8], refs[8:]
    two_rows, width = x_refs[0].shape
    rows = two_rows // 2
    core = place_ref[32]
    copies = {True: [], False: []}
    for n, (view, first, is_in, place, twin) in enumerate(parts):
        m = place_ref[16 + place]
        side = (1 - core) if twin else core
        if is_in:
            at = pl.multiple_of((2 * m + side) * W_IN_ROWS, W_IN_ROWS)
            target = w_in_ref.at[:, pl.ds(at, W_IN_ROWS), :]
            blocks = w_in_ref.shape[0]
        else:
            at = pl.multiple_of(m * W_OUT_ROWS, W_OUT_ROWS)
            target = w_out_ref.at[side, :, pl.ds(at, W_OUT_ROWS), :]
            blocks = w_out_ref.shape[1]
        copies[is_in].append(
            pltpu.make_async_copy(w_refs[view].at[pl.ds(first, blocks)], target, sems.at[n])
        )
    for is_in in (True, False):
        for copy in copies[is_in]:
            copy.start()
    for copy in copies[True]:
        copy.wait()
    pre = jnp.zeros((two_rows, w_in_ref.shape[0] * HEAD_DIM), jnp.float32)
    for n in range(8):
        at = pl.multiple_of(place_ref[n] * width, width)
        w = jnp.concatenate(
            [w_in_ref[j, pl.ds(at, width), :] for j in range(w_in_ref.shape[0])], axis=1
        )
        pre = pre + jnp.dot(x_refs[n][...], w, preferred_element_type=jnp.float32)
    hidden, d_hidden = gelu_pair(pre[:rows], pre[rows:])
    hidden = jnp.concatenate([hidden.astype(jnp.bfloat16), d_hidden.astype(jnp.bfloat16)], axis=0)
    for copy in copies[False]:
        copy.wait()
    each = width // HEAD_DIM
    per_side = w_out_ref.shape[1] // each
    for n in range(8):
        place = place_ref[8 + n]
        side, first = place // per_side, (place % per_side) * each
        w = jnp.concatenate([w_out_ref[side, first + t] for t in range(each)], axis=1)
        out = jnp.dot(hidden, w, preferred_element_type=jnp.float32)
        out_refs[n][...] = out.astype(jnp.bfloat16)


def whole():
    return pl.BlockSpec(memory_space=pltpu.VMEM)


W_IN_ROWS, W_OUT_ROWS = 96, 56


def gather_y(group, cut):
    up, down = shift(group, "y", 1), shift(group, "y", -1)
    return group, up, down, shift(up[:cut], "y", 1), shift(down[cut:], "y", -1)


def on_device(query, key, value, d_query, d_key, d_value, residual, d_residual, w_in, w_out):
    rows, width = query.shape
    core = lax.axis_index("c")
    bf16 = jnp.bfloat16
    steps = (1, -1, 2)

    w_out_twin = shift(w_out, "c", 1)
    qs = jnp.stack([query, d_query])
    q_pieces = [qs] + [shift(qs, "zh", s) for s in steps]
    kv = jnp.stack([key, value, d_key, d_value])
    kv_pieces = [kv] + [shift(kv, "y", s) for s in steps]
    kv_pieces = kv_pieces + [shift(piece, "c", 1) for piece in kv_pieces]

    one = W_IN_ROWS * (w_in.shape[1] // HEAD_DIM)
    packed = pl.pallas_call(
        pack_kernel,
        out_shape=jax.ShapeDtypeStruct((2 * one, HEAD_DIM), bf16),
        in_specs=[pl.BlockSpec(memory_space=pltpu.SMEM)] + [whole()] * 3,
        out_specs=whole(),
        compiler_params=pltpu.CompilerParams(vmem_limit_bytes=4 << 20),
        cost_estimate=pl.CostEstimate(flops=1_000_000, bytes_accessed=900_000, transcendentals=0),
        name="pack",
    )(core.astype(jnp.int32)[None], w_in, w_out, w_out_twin)
    low, high, far = (shift(packed, "zh", s) for s in steps)
    near = jnp.concatenate([low, high], axis=0)
    groups = ((packed, (0,), one), (near, (-1, 1), 2 * one), (far, (2,), one))
    arrays = []
    for group, dzs, cut in groups:
        halves = [(is_in, dz) for dz in dzs for is_in in (True, False)]
        pieces = gather_y(group, cut)
        contents = (
            [(i, 0, z) for i, z in halves],
            [(i, -1, z) for i, z in halves],
            [(i, 1, z) for i, z in halves],
            [(i, 2, z) for i, z in halves[: len(halves) // 2]],
            [(i, 2, z) for i, z in halves[len(halves) // 2 :]],
        )
        for piece, content in zip(pieces, contents):
            arrays.append((piece, content, False))
            arrays.append((shift(piece, "c", 1), content, True))
    views, parts = [], []
    for piece, content, twin in arrays:
        for is_in in (True, False):
            picked = [(n, c) for n, c in enumerate(content) if c[0] == is_in]
            if picked:
                tall = W_IN_ROWS if is_in else W_OUT_ROWS
                for n, (_, dy, dz) in picked:
                    place = (dy % NY) * NH + dz % NH
                    parts.append((len(views), n * (one // tall), is_in, place, twin))
                views.append(piece.reshape(-1, tall, HEAD_DIM))

    message = jax.ShapeDtypeStruct((2 * rows + STAT_ROWS, width), bf16)
    partial = pl.pallas_call(
        attend_kernel,
        out_shape=[message] * 4,
        in_specs=[whole()] * 12,
        out_specs=[whole()] * 4,
        compiler_params=pltpu.CompilerParams(vmem_limit_bytes=24 << 20),
        cost_estimate=pl.CostEstimate(
            flops=2_415_919_104, bytes_accessed=6_000_000, transcendentals=1_572_864
        ),
        name="attend",
    )(*q_pieces, *kv_pieces)
    partial = [partial[0]] + [shift(p, "zh", -s) for p, s in zip(partial[1:], steps)]
    x = pl.pallas_call(
        combine_kernel,
        out_shape=jax.ShapeDtypeStruct((2 * rows, width), bf16),
        in_specs=[whole()] * 6,
        out_specs=whole(),
        compiler_params=pltpu.CompilerParams(vmem_limit_bytes=6 << 20),
        cost_estimate=pl.CostEstimate(
            flops=2_000_000, bytes_accessed=1_300_000, transcendentals=2_000
        ),
        name="combine",
    )(*partial, residual, d_residual)

    px, pz = lax.axis_index("x"), lax.axis_index("zl")
    py, ph = lax.axis_index("y"), lax.axis_index("zh")
    place = jnp.stack(
        [((px - dx) % NX) * NL + (pz - dz) % NL for dx, dz in DP_STEPS]
        + [((px + dx) % NX) * NL + (pz + dz) % NL for dx, dz in DP_STEPS]
        + [((py + dy) % NY) * NH + (ph + dz) % NH for dy in range(NY) for dz in range(NH)]
        + [core]
    ).astype(jnp.int32)
    xs = [x] + [shift_dp(x, dx, dz) for dx, dz in DP_STEPS[1:]]
    sums = pl.pallas_call(
        functools.partial(feed_kernel, tuple(parts)),
        out_shape=[jax.ShapeDtypeStruct((2 * rows, width), bf16)] * 8,
        in_specs=[pl.BlockSpec(memory_space=pltpu.SMEM)]
        + [whole()] * 8
        + [pl.BlockSpec(memory_space=pl.ANY)] * len(views),
        out_specs=[whole()] * 8,
        scratch_shapes=[
            pltpu.VMEM((w_in.shape[1] // HEAD_DIM, 32 * W_IN_ROWS, HEAD_DIM), bf16),
            pltpu.VMEM((2, w_out.shape[1] // 2 // HEAD_DIM, 16 * W_OUT_ROWS, HEAD_DIM), bf16),
            pltpu.SemaphoreType.DMA((len(parts),)),
        ],
        compiler_params=pltpu.CompilerParams(vmem_limit_bytes=28 << 20),
        cost_estimate=pl.CostEstimate(
            flops=2_818_572_288, bytes_accessed=14_000_000, transcendentals=120_000
        ),
        name="feed",
    )(place, *xs, *views)
    sums = [sums[0]] + [shift_dp(s, dx, dz) for s, (dx, dz) in zip(sums[1:], DP_STEPS[1:])]
    total = x.astype(jnp.float32)
    for s in sums:
        total = total + s.astype(jnp.float32)
    total = total.astype(bf16)
    return (total[:rows], total[rows:])


def solution(mesh):
    fine = Mesh(mesh.devices.reshape(NX, NL, NY, NH, 2), ("x", "zl", "y", "zh", "c"))
    dp, seq = ("x", "zl"), ("y", "zh", "c")
    tokens = P(seq, dp)
    return jax.shard_map(
        on_device,
        mesh=fine,
        in_specs=(tokens,) * 9 + (P(dp + seq, None),),
        out_specs=(tokens, tokens),
        check_vma=False,
    )
```

```python
import functools
import math

import jax
import jax.numpy as jnp
from jax import lax
from jax.experimental import pallas as pl
from jax.experimental.pallas import tpu as pltpu
from jax.sharding import Mesh, PartitionSpec as P

HEAD_DIM = 128

gelu_coeff = 0.7978845608
cubic_coeff = 0.044715

NX, NL, NY, NH = 4, 2, 4, 4
STAT_ROWS = 8


def gelu_pair(pre_act, d_pre_act):
    inner_arg = gelu_coeff * (pre_act + cubic_coeff * pre_act * pre_act * pre_act)
    hyper = jnp.tanh(inner_arg)
    gelu_value = 0.5 * pre_act * (1.0 + hyper)
    gelu_slope = 0.5 * (1.0 + hyper) + 0.5 * pre_act * (1.0 - hyper * hyper) * gelu_coeff * (
        1.0 + 3.0 * cubic_coeff * pre_act * pre_act
    )
    return (gelu_value, gelu_slope * d_pre_act)


def shift(value, axis, step):
    size = lax.axis_size(axis)
    return lax.ppermute(value, axis, [(i, (i + step) % size) for i in range(size)])


def shift_dp(value, dx, dz):
    pairs = [
        (i * NL + j, ((i + dx) % NX) * NL + (j + dz) % NL) for i in range(NX) for j in range(NL)
    ]
    return lax.ppermute(value, ("x", "zl"), pairs)


DP_STEPS = [(dx, dz) for dx in range(NX) for dz in range(NL)]


def split3(value):
    high = value.astype(jnp.bfloat16).astype(jnp.float32)
    rest = value - high
    middle = rest.astype(jnp.bfloat16).astype(jnp.float32)
    return high, middle, rest - middle


def all_at_once(pairs, sems):
    copies = [pltpu.make_async_copy(a, b, sems.at[n]) for n, (a, b) in enumerate(pairs)]
    for copy in copies:
        copy.start()
    for copy in copies:
        copy.wait()


def finish_kernel(x_ref, sums_ref, out_ref, d_out_ref):
    rows = out_ref.shape[0]
    total = x_ref[...].astype(jnp.float32)
    for n in range(sums_ref.shape[0]):
        total = total + sums_ref[n].astype(jnp.float32)
    out_ref[...] = total[:rows].astype(jnp.bfloat16)
    d_out_ref[...] = total[rows:].astype(jnp.bfloat16)


def mark_kernel(_, out_ref):
    out_ref[...] = jnp.zeros_like(out_ref)


def attend_kernel(*refs):
    q_refs, kv_refs, out_refs = refs[:4], refs[4:12], refs[12:16]
    rows = q_refs[0].shape[1]
    scale = 1.0 / math.sqrt(HEAD_DIM)
    nt = (((1,), (1,)), ((), ()))

    def head(h, carry):
        at = pl.ds(pl.multiple_of(h * HEAD_DIM, HEAD_DIM), HEAD_DIM)
        k, v, dk, dv = (
            jnp.concatenate([ref[j, :, at] for ref in kv_refs], axis=0) for j in range(4)
        )
        k_dk = jnp.concatenate([k, dk], axis=1)
        v_dv = jnp.concatenate([v, dv], axis=1)
        for pair in range(2):
            ours = q_refs[2 * pair : 2 * pair + 2]
            q = jnp.concatenate([ref[0, :, at] for ref in ours], axis=0)
            dq = jnp.concatenate([ref[1, :, at] for ref in ours], axis=0)
            scores = lax.dot_general(q, k, nt, preferred_element_type=jnp.float32) * scale
            d_scores = lax.dot_general(
                jnp.concatenate([dq, q], axis=1), k_dk, nt, preferred_element_type=jnp.float32
            )
            d_scores = d_scores * scale
            peak = jnp.max(scores, axis=1, keepdims=True)
            weights = jnp.exp(scores - peak)
            mixed = weights * d_scores
            total = jnp.sum(weights, axis=1, keepdims=True)
            slope = jnp.sum(mixed, axis=1, keepdims=True)
            both = jnp.dot(weights.astype(jnp.bfloat16), v_dv, preferred_element_type=jnp.float32)
            tangent = both[:, HEAD_DIM:] + jnp.dot(
                mixed.astype(jnp.bfloat16), v, preferred_element_type=jnp.float32
            )
            share = 1.0 / total
            sigma = slope * share
            attended = both[:, :HEAD_DIM] * share
            d_attended = tangent * share - sigma * attended
            parts = split3(peak + jnp.log(total)) + split3(sigma)
            lane = lax.broadcasted_iota(jnp.int32, (2 * rows, HEAD_DIM), 1)
            table = jnp.zeros((2 * rows, HEAD_DIM), jnp.float32)
            for n, part in enumerate(parts):
                table = jnp.where(lane == n, part, table)
            for b in range(2):
                mine = slice(b * rows, (b + 1) * rows)
                out = out_refs[2 * pair + b]
                out[0:rows, at] = attended[mine].astype(jnp.bfloat16)
                out[rows : 2 * rows, at] = d_attended[mine].astype(jnp.bfloat16)
                out[2 * rows : 2 * rows + STAT_ROWS, at] = table[mine].T[:STAT_ROWS].astype(
                    jnp.bfloat16
                )
        return carry

    lax.fori_loop(0, q_refs[0].shape[2] // HEAD_DIM, head, 0)


def combine_kernel(*refs):
    part_refs, res_ref, dres_ref, out_ref = refs[:4], refs[4], refs[5], refs[6]
    rows = res_ref.shape[0]
    heads = res_ref.shape[1] // HEAD_DIM
    table = []
    for h in range(heads):
        at = slice(h * HEAD_DIM, (h + 1) * HEAD_DIM)
        stats = [ref[2 * rows : 2 * rows + STAT_ROWS, at].astype(jnp.float32) for ref in part_refs]
        logs = [s[0:1] + s[1:2] + s[2:3] for s in stats]
        sigmas = [s[3:4] + s[4:5] + s[5:6] for s in stats]
        peak = functools.reduce(jnp.maximum, logs)
        shares = [jnp.exp(log - peak) for log in logs]
        norm = 1.0 / sum(shares)
        shares = [share * norm for share in shares]
        sigma = sum(p * s for p, s in zip(shares, sigmas))
        table += shares + [p * (s - sigma) for p, s in zip(shares, sigmas)]
    table.append(jnp.zeros((HEAD_DIM - 8 * heads, rows), jnp.float32))
    table = jnp.concatenate(table, axis=0).T
    for h in range(heads):
        at = slice(h * HEAD_DIM, (h + 1) * HEAD_DIM)
        attended = jnp.zeros((rows, HEAD_DIM), jnp.float32)
        d_attended = jnp.zeros((rows, HEAD_DIM), jnp.float32)
        for n, ref in enumerate(part_refs):
            a = ref[0:rows, at].astype(jnp.float32)
            d = ref[rows : 2 * rows, at].astype(jnp.float32)
            p = table[:, 8 * h + n : 8 * h + n + 1]
            r = table[:, 8 * h + 4 + n : 8 * h + 5 + n]
            attended = attended + p * a
            d_attended = d_attended + (p * d + r * a)
        mixed = res_ref[:, at].astype(jnp.float32) + attended
        d_mixed = dres_ref[:, at].astype(jnp.float32) + d_attended
        out_ref[0:rows, at] = mixed.astype(jnp.bfloat16)
        out_ref[rows : 2 * rows, at] = d_mixed.astype(jnp.bfloat16)


def pack_kernel(core_ref, w_in_hbm, w_out_hbm, twin_ref, out_ref, w_in_ref, w_out_ref, sems):
    all_at_once([(w_in_hbm, w_in_ref), (w_out_hbm, w_out_ref)], sems)
    own, width = w_in_ref.shape
    few, half = w_out_ref.shape[0], w_out_ref.shape[1] // 2
    lanes = HEAD_DIM
    for j in range(width // lanes):
        out_ref[j * own : (j + 1) * own] = w_in_ref[:, j * lanes : (j + 1) * lanes]
    base = own * (width // lanes)
    for core in range(2):

        @pl.when(core_ref[0] == core)
        def _():
            pair = (w_out_ref, twin_ref) if core == 0 else (twin_ref, w_out_ref)
            for j in range(half // lanes):
                at = slice(core * half + j * lanes, core * half + (j + 1) * lanes)
                block = jnp.concatenate([ref[:, at].astype(jnp.float32) for ref in pair], axis=0)
                start = base + j * 2 * few
                out_ref[start : start + 2 * few] = block.astype(jnp.bfloat16)


def join_kernel(*refs):
    parts, out_ref, sems = refs[:-2], refs[-2], refs[-1]
    copies, at = [], 0
    for n, ref in enumerate(parts):
        copies.append(
            pltpu.make_async_copy(ref, out_ref.at[pl.ds(at, ref.shape[0])], sems.at[n])
        )
        at += ref.shape[0]
    for copy in copies:
        copy.start()
    for copy in copies:
        copy.wait()


def join(arrays):
    rows = sum(array.shape[0] for array in arrays)
    size = 2 * rows * HEAD_DIM
    return pl.pallas_call(
        join_kernel,
        out_shape=jax.ShapeDtypeStruct((rows, HEAD_DIM), jnp.bfloat16),
        in_specs=[pl.BlockSpec(memory_space=pl.ANY)] * len(arrays),
        out_specs=whole(),
        scratch_shapes=[pltpu.SemaphoreType.DMA((len(arrays),))],
        compiler_params=pltpu.CompilerParams(vmem_limit_bytes=size + (1 << 20)),
        cost_estimate=pl.CostEstimate(flops=1000, bytes_accessed=2 * size, transcendentals=0),
        name="join",
    )(*arrays)


def assemble_kernel(parts, place_ref, *refs):
    w_refs, (w_in_ref, w_out_ref, sems) = refs[: 1 + max(view for view, *_ in parts)], refs[-3:]
    core = place_ref[32]
    copies = []
    for n, (view, first, is_in, place, twin) in enumerate(parts):
        m = place_ref[16 + place]
        side = (1 - core) if twin else core
        if is_in:
            at = pl.multiple_of((2 * m + side) * W_IN_ROWS, W_IN_ROWS)
            target = w_in_ref.at[:, pl.ds(at, W_IN_ROWS), :]
            blocks = w_in_ref.shape[0]
        else:
            at = pl.multiple_of(m * W_OUT_ROWS, W_OUT_ROWS)
            target = w_out_ref.at[side, :, pl.ds(at, W_OUT_ROWS), :]
            blocks = w_out_ref.shape[1]
        copies.append(
            pltpu.make_async_copy(w_refs[view].at[pl.ds(first, blocks)], target, sems.at[n])
        )
    for copy in copies:
        copy.start()
    for copy in copies:
        copy.wait()


def feed_kernel(place_ref, *refs):
    x_refs, (w_in_ref, w_out_ref, out_ref, x_ref, hid_ref) = refs[:8], refs[8:]
    two_rows, width = x_refs[0].shape
    rows = two_rows // 2
    for n in range(8):
        x_ref[:, pl.ds(pl.multiple_of(place_ref[n] * width, width), width)] = x_refs[n][...]
    blocks = w_in_ref.shape[0]

    def onto(j, count):
        w = jnp.concatenate([w_in_ref[j + t] for t in range(count)], axis=1)
        pre = jnp.dot(x_ref[...], w, preferred_element_type=jnp.float32)
        hidden, d_hidden = gelu_pair(pre[:rows], pre[rows:])
        at = pl.ds(pl.multiple_of(j * HEAD_DIM, HEAD_DIM), count * HEAD_DIM)
        hid_ref[:rows, at] = hidden.astype(jnp.bfloat16)
        hid_ref[rows:, at] = d_hidden.astype(jnp.bfloat16)

    lax.fori_loop(0, blocks // 2, lambda n, c: (onto(2 * n, 2), c)[1], 0)
    onto(blocks - 1, 1)
    each = width // HEAD_DIM
    per_side = w_out_ref.shape[1] // each

    def out_of(n, carry):
        first = (n % per_side) * each
        w = jnp.concatenate([w_out_ref[n // per_side, first + t] for t in range(each)], axis=1)
        out = jnp.dot(hid_ref[...], w, preferred_element_type=jnp.float32)
        out_ref[n] = out.astype(jnp.bfloat16)
        return carry

    lax.fori_loop(0, 8, out_of, 0)


def whole():
    return pl.BlockSpec(memory_space=pltpu.VMEM)


W_IN_ROWS, W_OUT_ROWS = 96, 56


def on_device(query, key, value, d_query, d_key, d_value, residual, d_residual, w_in, w_out):
    rows, width = query.shape
    core = lax.axis_index("c")
    bf16 = jnp.bfloat16
    steps = (1, -1, 2)

    w_out_twin = shift(w_out, "c", 1)
    qs = jnp.stack([query, d_query])
    kv = jnp.stack([key, value, d_key, d_value])
    q_pieces = [qs] + [shift(qs, "zh", st) for st in steps]
    kv_pieces = [kv] + [shift(kv, "y", st) for st in steps]
    kv_pieces = kv_pieces + [shift(p, "c", 1) for p in kv_pieces]

    one = W_IN_ROWS * (w_in.shape[1] // HEAD_DIM)
    packed = pl.pallas_call(
        pack_kernel,
        out_shape=jax.ShapeDtypeStruct((2 * one, HEAD_DIM), bf16),
        in_specs=[pl.BlockSpec(memory_space=pltpu.SMEM)]
        + [pl.BlockSpec(memory_space=pltpu.HBM)] * 2
        + [whole()],
        out_specs=whole(),
        scratch_shapes=[
            pltpu.VMEM(w_in.shape, bf16),
            pltpu.VMEM(w_out.shape, bf16),
            pltpu.SemaphoreType.DMA((2,)),
        ],
        compiler_params=pltpu.CompilerParams(vmem_limit_bytes=4 << 20),
        cost_estimate=pl.CostEstimate(flops=1_000_000, bytes_accessed=900_000, transcendentals=0),
        name="pack",
    )(core.astype(jnp.int32)[None], w_in, w_out, w_out_twin)
    low, high = (shift(packed, "zh", st) for st in steps[:2])
    ways = (1, -1, 2)
    own = [shift(packed, "y", st) for st in ways]
    far_a, far_b = shift(low[:one], "zh", 1), shift(high[one:], "zh", -1)
    near = jnp.concatenate([low, high], axis=0)
    up, down = (shift(near, "y", st) for st in (1, -1))
    message = jax.ShapeDtypeStruct((2 * rows + STAT_ROWS, width), bf16)
    attend = pl.pallas_call(
        attend_kernel,
        out_shape=[message] * 4,
        in_specs=[whole()] * 12,
        out_specs=[whole()] * 4,
        compiler_params=pltpu.CompilerParams(vmem_limit_bytes=24 << 20),
        cost_estimate=pl.CostEstimate(
            flops=2_415_919_104, bytes_accessed=6_000_000, transcendentals=1_572_864
        ),
        name="attend",
    )
    partial = attend(*q_pieces, *kv_pieces)
    mark = pl.pallas_call(
        mark_kernel,
        out_shape=jax.ShapeDtypeStruct((8, HEAD_DIM), jnp.float32),
        in_specs=[pl.BlockSpec(memory_space=pl.ANY)],
        out_specs=whole(),
        compiler_params=pltpu.CompilerParams(
            vmem_limit_bytes=1 << 20, has_side_effects=True
        ),
        name="mark",
    )(partial[0])
    far_a, far_b, up, down, _ = lax.optimization_barrier((far_a, far_b, up, down, mark))
    partial = [partial[0]] + [shift(p, "zh", -st) for p, st in zip(partial[1:], steps)]
    combine = pl.pallas_call(
        combine_kernel,
        out_shape=jax.ShapeDtypeStruct((2 * rows, width), bf16),
        in_specs=[whole()] * 6,
        out_specs=whole(),
        compiler_params=pltpu.CompilerParams(vmem_limit_bytes=6 << 20),
        cost_estimate=pl.CostEstimate(
            flops=2_000_000, bytes_accessed=1_300_000, transcendentals=2_000
        ),
        name="combine",
    )
    x = combine(*partial, residual, d_residual)

    far = join([far_a, far_b])
    far_out = [shift(far, "y", st) for st in ways]
    far_a = shift(up[: 2 * one], "y", 1)
    far_b = shift(down[2 * one :], "y", -1)
    up, down, *own, _ = lax.optimization_barrier((up, down, *own, x))
    far_a, far_b, *far_out, _ = lax.optimization_barrier((far_a, far_b, *far_out, x))
    early = join([packed, *own, near, up, down])
    early_places = [(0, 0), (-1, 0), (1, 0), (2, 0)]
    early_places += [(0, -1), (0, 1), (-1, -1), (-1, 1), (1, -1), (1, 1)]
    late = join([far, *far_out, far_a, far_b])
    late_places = [(0, 2), (-1, 2), (1, 2), (2, 2), (2, -1), (2, 1)]

    def views_of(array, places):
        views, parts = [], []
        for piece, twin in ((array, False), (shift(array, "c", 1), True)):
            for is_in, tall in ((True, W_IN_ROWS), (False, W_OUT_ROWS)):
                skip = 0 if is_in else one // tall
                for n, (dy, dz) in enumerate(places):
                    first = n * (2 * one // tall) + skip
                    parts.append((len(views), first, is_in, (dy % NY) * NH + dz % NH, twin))
                views.append(piece.reshape(-1, tall, HEAD_DIM))
        return views, tuple(parts)

    px, pz = lax.axis_index("x"), lax.axis_index("zl")
    py, ph = lax.axis_index("y"), lax.axis_index("zh")
    place = jnp.stack(
        [((px - dx) % NX) * NL + (pz - dz) % NL for dx, dz in DP_STEPS]
        + [0] * 8
        + [((py + dy) % NY) * NH + (ph + dz) % NH for dy in range(NY) for dz in range(NH)]
        + [core]
    ).astype(jnp.int32)
    xs = [x] + [shift_dp(x, dx, dz) for dx, dz in DP_STEPS[1:]]
    shapes = [
        jax.ShapeDtypeStruct((w_in.shape[1] // HEAD_DIM, 32 * W_IN_ROWS, HEAD_DIM), bf16),
        jax.ShapeDtypeStruct((2, w_out.shape[1] // 2 // HEAD_DIM, 16 * W_OUT_ROWS, HEAD_DIM), bf16),
    ]
    built = []
    for array, places in ((early, early_places), (late, late_places)):
        views, parts = views_of(array, places)
        assemble = pl.pallas_call(
            functools.partial(assemble_kernel, parts),
            out_shape=shapes,
            in_specs=[pl.BlockSpec(memory_space=pltpu.SMEM)]
            + [pl.BlockSpec(memory_space=pl.ANY)] * len(views)
            + [whole()] * len(built),
            out_specs=[whole()] * 2,
            scratch_shapes=[pltpu.SemaphoreType.DMA((len(parts),))],
            input_output_aliases={1 + len(views) + n: n for n in range(len(built))},
            compiler_params=pltpu.CompilerParams(vmem_limit_bytes=13 << 20),
            cost_estimate=pl.CostEstimate(
                flops=1_000_000_000, bytes_accessed=11_000_000, transcendentals=0
            ),
            name="assemble",
        )
        built = assemble(place, *views, *built)
    w_in_whole, w_out_whole = built
    sums = pl.pallas_call(
        feed_kernel,
        out_shape=jax.ShapeDtypeStruct((8, 2 * rows, width), bf16),
        in_specs=[pl.BlockSpec(memory_space=pltpu.SMEM)] + [whole()] * 10,
        out_specs=whole(),
        scratch_shapes=[
            pltpu.VMEM((2 * rows, 8 * width), bf16),
            pltpu.VMEM((2 * rows, w_in.shape[1]), bf16),
        ],
        compiler_params=pltpu.CompilerParams(vmem_limit_bytes=22 << 20),
        cost_estimate=pl.CostEstimate(
            flops=2_818_572_288, bytes_accessed=14_000_000, transcendentals=120_000
        ),
        name="feed",
    )(place, *xs, w_in_whole, w_out_whole)
    sums = lax.all_to_all(sums, ("x", "zl"), 0, 0, tiled=True)
    return tuple(
        pl.pallas_call(
            finish_kernel,
            out_shape=[jax.ShapeDtypeStruct((rows, width), bf16)] * 2,
            in_specs=[whole()] * 2,
            out_specs=[whole()] * 2,
            compiler_params=pltpu.CompilerParams(vmem_limit_bytes=8 << 20),
            cost_estimate=pl.CostEstimate(
                flops=1_000_000, bytes_accessed=2_000_000, transcendentals=0
            ),
            name="finish",
        )(x, sums)
    )


def solution(mesh):
    fine = Mesh(mesh.devices.reshape(NX, NL, NY, NH, 2), ("x", "zl", "y", "zh", "c"))
    dp, seq = ("x", "zl"), ("y", "zh", "c")
    tokens = P(seq, dp)
    return jax.shard_map(
        on_device,
        mesh=fine,
        in_specs=(tokens,) * 9 + (P(dp + seq, None),),
        out_specs=(tokens, tokens),
        check_vma=False,
    )
```

```python
import functools
import math

import jax
import jax.numpy as jnp
from jax import lax
from jax.experimental import pallas as pl
from jax.experimental.pallas import tpu as pltpu
from jax.sharding import Mesh, PartitionSpec as P

HEAD_DIM = 128

gelu_coeff = 0.7978845608
cubic_coeff = 0.044715

NX, NL, NY, NH = 4, 2, 4, 4
STAT_ROWS = 8


def gelu_pair(pre_act, d_pre_act):
    inner_arg = gelu_coeff * (pre_act + cubic_coeff * pre_act * pre_act * pre_act)
    hyper = jnp.tanh(inner_arg)
    gelu_value = 0.5 * pre_act * (1.0 + hyper)
    gelu_slope = 0.5 * (1.0 + hyper) + 0.5 * pre_act * (1.0 - hyper * hyper) * gelu_coeff * (
        1.0 + 3.0 * cubic_coeff * pre_act * pre_act
    )
    return (gelu_value, gelu_slope * d_pre_act)


def shift(value, axis, step):
    size = lax.axis_size(axis)
    return lax.ppermute(value, axis, [(i, (i + step) % size) for i in range(size)])


def shift_dp(value, dx, dz):
    pairs = [
        (i * NL + j, ((i + dx) % NX) * NL + (j + dz) % NL) for i in range(NX) for j in range(NL)
    ]
    return lax.ppermute(value, ("x", "zl"), pairs)


DP_STEPS = [(dx, dz) for dx in range(NX) for dz in range(NL)]


def split3(value):
    high = value.astype(jnp.bfloat16).astype(jnp.float32)
    rest = value - high
    middle = rest.astype(jnp.bfloat16).astype(jnp.float32)
    return high, middle, rest - middle


def all_at_once(pairs, sems):
    copies = [pltpu.make_async_copy(a, b, sems.at[n]) for n, (a, b) in enumerate(pairs)]
    for copy in copies:
        copy.start()
    for copy in copies:
        copy.wait()


def finish_kernel(x_ref, sums_ref, out_ref, d_out_ref):
    rows = out_ref.shape[0]
    total = x_ref[...].astype(jnp.float32)
    for n in range(sums_ref.shape[0]):
        total = total + sums_ref[n].astype(jnp.float32)
    out_ref[...] = total[:rows].astype(jnp.bfloat16)
    d_out_ref[...] = total[rows:].astype(jnp.bfloat16)


def mark_kernel(*_):
    pass


def mark(array):
    return pl.pallas_call(
        mark_kernel,
        out_shape=jax.ShapeDtypeStruct((8, HEAD_DIM), jnp.float32),
        in_specs=[pl.BlockSpec(memory_space=pl.ANY)],
        out_specs=pl.BlockSpec(memory_space=pl.ANY),
        compiler_params=pltpu.CompilerParams(
            vmem_limit_bytes=1 << 20, has_side_effects=True
        ),
        name="mark",
    )(array)


def attend_kernel(*refs):
    q_refs, kv_refs, out_refs = refs[:4], refs[4:12], refs[12:16]
    rows = q_refs[0].shape[1]
    scale = 1.0 / math.sqrt(HEAD_DIM)
    nt = (((1,), (1,)), ((), ()))

    def head(h, carry):
        at = pl.ds(pl.multiple_of(h * HEAD_DIM, HEAD_DIM), HEAD_DIM)
        k, v, dk, dv = (
            jnp.concatenate([ref[j, :, at] for ref in kv_refs], axis=0) for j in range(4)
        )
        k_dk = jnp.concatenate([k, dk], axis=1)
        v_dv = jnp.concatenate([v, dv], axis=1)
        for pair in range(2):
            ours = q_refs[2 * pair : 2 * pair + 2]
            q = jnp.concatenate([ref[0, :, at] for ref in ours], axis=0)
            dq = jnp.concatenate([ref[1, :, at] for ref in ours], axis=0)
            scores = lax.dot_general(q, k, nt, preferred_element_type=jnp.float32) * scale
            d_scores = lax.dot_general(
                jnp.concatenate([dq, q], axis=1), k_dk, nt, preferred_element_type=jnp.float32
            )
            d_scores = d_scores * scale
            peak = jnp.max(scores, axis=1, keepdims=True)
            weights = jnp.exp(scores - peak)
            mixed = weights * d_scores
            total = jnp.sum(weights, axis=1, keepdims=True)
            slope = jnp.sum(mixed, axis=1, keepdims=True)
            both = jnp.dot(weights.astype(jnp.bfloat16), v_dv, preferred_element_type=jnp.float32)
            tangent = both[:, HEAD_DIM:] + jnp.dot(
                mixed.astype(jnp.bfloat16), v, preferred_element_type=jnp.float32
            )
            share = 1.0 / total
            sigma = slope * share
            attended = both[:, :HEAD_DIM] * share
            d_attended = tangent * share - sigma * attended
            parts = split3(peak + jnp.log(total)) + split3(sigma)
            lane = lax.broadcasted_iota(jnp.int32, (2 * rows, HEAD_DIM), 1)
            table = jnp.zeros((2 * rows, HEAD_DIM), jnp.float32)
            for n, part in enumerate(parts):
                table = jnp.where(lane == n, part, table)
            for b in range(2):
                mine = slice(b * rows, (b + 1) * rows)
                out = out_refs[2 * pair + b]
                out[0:rows, at] = attended[mine].astype(jnp.bfloat16)
                out[rows : 2 * rows, at] = d_attended[mine].astype(jnp.bfloat16)
                out[2 * rows : 2 * rows + STAT_ROWS, at] = table[mine].T[:STAT_ROWS].astype(
                    jnp.bfloat16
                )
        return carry

    lax.fori_loop(0, q_refs[0].shape[2] // HEAD_DIM, head, 0)


def combine_kernel(*refs):
    part_refs, res_ref, dres_ref, out_ref = refs[:4], refs[4], refs[5], refs[6]
    rows = res_ref.shape[0]
    heads = res_ref.shape[1] // HEAD_DIM
    table = []
    for h in range(heads):
        at = slice(h * HEAD_DIM, (h + 1) * HEAD_DIM)
        stats = [ref[2 * rows : 2 * rows + STAT_ROWS, at].astype(jnp.float32) for ref in part_refs]
        logs = [s[0:1] + s[1:2] + s[2:3] for s in stats]
        sigmas = [s[3:4] + s[4:5] + s[5:6] for s in stats]
        peak = functools.reduce(jnp.maximum, logs)
        shares = [jnp.exp(log - peak) for log in logs]
        norm = 1.0 / sum(shares)
        shares = [share * norm for share in shares]
        sigma = sum(p * s for p, s in zip(shares, sigmas))
        table += shares + [p * (s - sigma) for p, s in zip(shares, sigmas)]
    table.append(jnp.zeros((HEAD_DIM - 8 * heads, rows), jnp.float32))
    table = jnp.concatenate(table, axis=0).T
    for h in range(heads):
        at = slice(h * HEAD_DIM, (h + 1) * HEAD_DIM)
        attended = jnp.zeros((rows, HEAD_DIM), jnp.float32)
        d_attended = jnp.zeros((rows, HEAD_DIM), jnp.float32)
        for n, ref in enumerate(part_refs):
            a = ref[0:rows, at].astype(jnp.float32)
            d = ref[rows : 2 * rows, at].astype(jnp.float32)
            p = table[:, 8 * h + n : 8 * h + n + 1]
            r = table[:, 8 * h + 4 + n : 8 * h + 5 + n]
            attended = attended + p * a
            d_attended = d_attended + (p * d + r * a)
        mixed = res_ref[:, at].astype(jnp.float32) + attended
        d_mixed = dres_ref[:, at].astype(jnp.float32) + d_attended
        out_ref[0:rows, at] = mixed.astype(jnp.bfloat16)
        out_ref[rows : 2 * rows, at] = d_mixed.astype(jnp.bfloat16)


def pack_kernel(core_ref, w_in_hbm, w_out_hbm, twin_ref, out_ref, w_in_ref, w_out_ref, sems):
    all_at_once([(w_in_hbm, w_in_ref), (w_out_hbm, w_out_ref)], sems)
    own, width = w_in_ref.shape
    few, half = w_out_ref.shape[0], w_out_ref.shape[1] // 2
    lanes = HEAD_DIM
    for j in range(width // lanes):
        out_ref[j * own : (j + 1) * own] = w_in_ref[:, j * lanes : (j + 1) * lanes]
    base = own * (width // lanes)
    for core in range(2):

        @pl.when(core_ref[0] == core)
        def _():
            pair = (w_out_ref, twin_ref) if core == 0 else (twin_ref, w_out_ref)
            for j in range(half // lanes):
                at = slice(core * half + j * lanes, core * half + (j + 1) * lanes)
                block = jnp.concatenate([ref[:, at].astype(jnp.float32) for ref in pair], axis=0)
                start = base + j * 2 * few
                out_ref[start : start + 2 * few] = block.astype(jnp.bfloat16)


def join_kernel(*refs):
    parts, out_ref, sems = refs[:-2], refs[-2], refs[-1]
    copies, at = [], 0
    for n, ref in enumerate(parts):
        copies.append(
            pltpu.make_async_copy(ref, out_ref.at[pl.ds(at, ref.shape[0])], sems.at[n])
        )
        at += ref.shape[0]
    for copy in copies:
        copy.start()
    for copy in copies:
        copy.wait()


def join(arrays):
    rows = sum(array.shape[0] for array in arrays)
    size = 2 * rows * HEAD_DIM
    return pl.pallas_call(
        join_kernel,
        out_shape=jax.ShapeDtypeStruct((rows, HEAD_DIM), jnp.bfloat16),
        in_specs=[pl.BlockSpec(memory_space=pl.ANY)] * len(arrays),
        out_specs=whole(),
        scratch_shapes=[pltpu.SemaphoreType.DMA((len(arrays),))],
        compiler_params=pltpu.CompilerParams(vmem_limit_bytes=size + (1 << 20)),
        cost_estimate=pl.CostEstimate(flops=1000, bytes_accessed=2 * size, transcendentals=0),
        name="join",
    )(*arrays)


def assemble_kernel(parts, place_ref, *refs):
    w_refs, (w_in_ref, w_out_ref, sems) = refs[: 1 + max(view for view, *_ in parts)], refs[-3:]
    core = place_ref[32]
    copies = []
    for n, (view, first, is_in, place, twin) in enumerate(parts):
        m = place_ref[16 + place]
        side = (1 - core) if twin else core
        if is_in:
            at = pl.multiple_of((2 * m + side) * W_IN_ROWS, W_IN_ROWS)
            target = w_in_ref.at[:, pl.ds(at, W_IN_ROWS), :]
            blocks = w_in_ref.shape[0]
        else:
            at = pl.multiple_of(m * W_OUT_ROWS, W_OUT_ROWS)
            target = w_out_ref.at[side, :, pl.ds(at, W_OUT_ROWS), :]
            blocks = w_out_ref.shape[1]
        copies.append(
            pltpu.make_async_copy(w_refs[view].at[pl.ds(first, blocks)], target, sems.at[n])
        )
    for copy in copies:
        copy.start()
    for copy in copies:
        copy.wait()


def feed_kernel(place_ref, *refs):
    x_refs, (w_in_ref, w_out_ref, out_ref, x_ref, hid_ref) = refs[:8], refs[8:]
    two_rows, width = x_refs[0].shape
    rows = two_rows // 2
    for n in range(8):
        x_ref[:, pl.ds(pl.multiple_of(place_ref[n] * width, width), width)] = x_refs[n][...]
    blocks = w_in_ref.shape[0]

    def onto(j, count):
        w = jnp.concatenate([w_in_ref[j + t] for t in range(count)], axis=1)
        pre = jnp.dot(x_ref[...], w, preferred_element_type=jnp.float32)
        hidden, d_hidden = gelu_pair(pre[:rows], pre[rows:])
        at = pl.ds(pl.multiple_of(j * HEAD_DIM, HEAD_DIM), count * HEAD_DIM)
        hid_ref[:rows, at] = hidden.astype(jnp.bfloat16)
        hid_ref[rows:, at] = d_hidden.astype(jnp.bfloat16)

    lax.fori_loop(0, blocks // 2, lambda n, c: (onto(2 * n, 2), c)[1], 0)
    onto(blocks - 1, 1)
    each = width // HEAD_DIM
    per_side = w_out_ref.shape[1] // each

    def out_of(n, carry):
        first = (n % per_side) * each
        w = jnp.concatenate([w_out_ref[n // per_side, first + t] for t in range(each)], axis=1)
        out = jnp.dot(hid_ref[...], w, preferred_element_type=jnp.float32)
        out_ref[n] = out.astype(jnp.bfloat16)
        return carry

    lax.fori_loop(0, 8, out_of, 0)


def whole():
    return pl.BlockSpec(memory_space=pltpu.VMEM)


W_IN_ROWS, W_OUT_ROWS = 96, 56


def on_device(query, key, value, d_query, d_key, d_value, residual, d_residual, w_in, w_out):
    rows, width = query.shape
    core = lax.axis_index("c")
    bf16 = jnp.bfloat16
    steps = (1, -1, 2)

    w_out_twin = shift(w_out, "c", 1)
    qs = jnp.stack([query, d_query])
    kv = jnp.stack([key, value, d_key, d_value])
    q_pieces = [qs] + [shift(qs, "zh", st) for st in steps]
    kv_pieces = [kv] + [shift(kv, "y", st) for st in steps]
    kv_pieces = kv_pieces + [shift(p, "c", 1) for p in kv_pieces]

    one = W_IN_ROWS * (w_in.shape[1] // HEAD_DIM)
    packed = pl.pallas_call(
        pack_kernel,
        out_shape=jax.ShapeDtypeStruct((2 * one, HEAD_DIM), bf16),
        in_specs=[pl.BlockSpec(memory_space=pltpu.SMEM)]
        + [pl.BlockSpec(memory_space=pltpu.HBM)] * 2
        + [whole()],
        out_specs=whole(),
        scratch_shapes=[
            pltpu.VMEM(w_in.shape, bf16),
            pltpu.VMEM(w_out.shape, bf16),
            pltpu.SemaphoreType.DMA((2,)),
        ],
        compiler_params=pltpu.CompilerParams(vmem_limit_bytes=4 << 20),
        cost_estimate=pl.CostEstimate(flops=1_000_000, bytes_accessed=900_000, transcendentals=0),
        name="pack",
    )(core.astype(jnp.int32)[None], w_in, w_out, w_out_twin)
    low, high = (shift(packed, "zh", st) for st in steps[:2])
    ways = (1, -1, 2)
    own = [shift(packed, "y", st) for st in ways]
    far_a, far_b = shift(low[:one], "zh", 1), shift(high[one:], "zh", -1)
    near = jnp.concatenate([low, high], axis=0)
    up, down = (shift(near, "y", st) for st in (1, -1))
    message = jax.ShapeDtypeStruct((2 * rows + STAT_ROWS, width), bf16)
    attend = pl.pallas_call(
        attend_kernel,
        out_shape=[message] * 4,
        in_specs=[whole()] * 12,
        out_specs=[whole()] * 4,
        compiler_params=pltpu.CompilerParams(vmem_limit_bytes=24 << 20),
        cost_estimate=pl.CostEstimate(
            flops=2_415_919_104, bytes_accessed=6_000_000, transcendentals=1_572_864
        ),
        name="attend",
    )
    partial = attend(*q_pieces, *kv_pieces)
    sent = mark(partial[0])
    far_a, far_b, _ = lax.optimization_barrier((far_a, far_b, sent))
    partial = [partial[0]] + [shift(p, "zh", -st) for p, st in zip(partial[1:], steps)]
    combine = pl.pallas_call(
        combine_kernel,
        out_shape=jax.ShapeDtypeStruct((2 * rows, width), bf16),
        in_specs=[whole()] * 6,
        out_specs=whole(),
        compiler_params=pltpu.CompilerParams(vmem_limit_bytes=6 << 20),
        cost_estimate=pl.CostEstimate(
            flops=2_000_000, bytes_accessed=1_300_000, transcendentals=2_000
        ),
        name="combine",
    )
    x = combine(*partial, residual, d_residual)

    far = join([far_a, far_b])
    far_out = [shift(far, "y", st) for st in ways]
    up, down, _ = lax.optimization_barrier((up, down, mark(far)))
    far_a = shift(up[: 2 * one], "y", 1)
    far_b = shift(down[2 * one :], "y", -1)
    up, down, *own, _ = lax.optimization_barrier((up, down, *own, x))
    posted = mark(x)
    far_a, far_b, *far_out, _ = lax.optimization_barrier((far_a, far_b, *far_out, posted))
    early = join([packed, *own, near, up, down])
    early_places = [(0, 0), (-1, 0), (1, 0), (2, 0)]
    early_places += [(0, -1), (0, 1), (-1, -1), (-1, 1), (1, -1), (1, 1)]
    late = join([far, *far_out, far_a, far_b])
    late_places = [(0, 2), (-1, 2), (1, 2), (2, 2), (2, -1), (2, 1)]

    def views_of(array, places):
        views, parts = [], []
        for piece, twin in ((array, False), (shift(array, "c", 1), True)):
            for is_in, tall in ((True, W_IN_ROWS), (False, W_OUT_ROWS)):
                skip = 0 if is_in else one // tall
                for n, (dy, dz) in enumerate(places):
                    first = n * (2 * one // tall) + skip
                    parts.append((len(views), first, is_in, (dy % NY) * NH + dz % NH, twin))
                views.append(piece.reshape(-1, tall, HEAD_DIM))
        return views, tuple(parts)

    px, pz = lax.axis_index("x"), lax.axis_index("zl")
    py, ph = lax.axis_index("y"), lax.axis_index("zh")
    place = jnp.stack(
        [((px - dx) % NX) * NL + (pz - dz) % NL for dx, dz in DP_STEPS]
        + [0] * 8
        + [((py + dy) % NY) * NH + (ph + dz) % NH for dy in range(NY) for dz in range(NH)]
        + [core]
    ).astype(jnp.int32)
    xs = [x] + [shift_dp(x, dx, dz) for dx, dz in DP_STEPS[1:]]
    shapes = [
        jax.ShapeDtypeStruct((w_in.shape[1] // HEAD_DIM, 32 * W_IN_ROWS, HEAD_DIM), bf16),
        jax.ShapeDtypeStruct((2, w_out.shape[1] // 2 // HEAD_DIM, 16 * W_OUT_ROWS, HEAD_DIM), bf16),
    ]
    built = []
    for array, places in ((early, early_places), (late, late_places)):
        views, parts = views_of(array, places)
        assemble = pl.pallas_call(
            functools.partial(assemble_kernel, parts),
            out_shape=shapes,
            in_specs=[pl.BlockSpec(memory_space=pltpu.SMEM)]
            + [pl.BlockSpec(memory_space=pl.ANY)] * len(views)
            + [whole()] * len(built),
            out_specs=[whole()] * 2,
            scratch_shapes=[pltpu.SemaphoreType.DMA((len(parts),))],
            input_output_aliases={1 + len(views) + n: n for n in range(len(built))},
            compiler_params=pltpu.CompilerParams(vmem_limit_bytes=13 << 20),
            cost_estimate=pl.CostEstimate(
                flops=1_000_000_000, bytes_accessed=11_000_000, transcendentals=0
            ),
            name="assemble",
        )
        built = assemble(place, *views, *built)
    w_in_whole, w_out_whole = built
    sums = pl.pallas_call(
        feed_kernel,
        out_shape=jax.ShapeDtypeStruct((8, 2 * rows, width), bf16),
        in_specs=[pl.BlockSpec(memory_space=pltpu.SMEM)] + [whole()] * 10,
        out_specs=whole(),
        scratch_shapes=[
            pltpu.VMEM((2 * rows, 8 * width), bf16),
            pltpu.VMEM((2 * rows, w_in.shape[1]), bf16),
        ],
        compiler_params=pltpu.CompilerParams(vmem_limit_bytes=22 << 20),
        cost_estimate=pl.CostEstimate(
            flops=2_818_572_288, bytes_accessed=14_000_000, transcendentals=120_000
        ),
        name="feed",
    )(place, *xs, w_in_whole, w_out_whole)
    sums = lax.all_to_all(sums, ("x", "zl"), 0, 0, tiled=True)
    return tuple(
        pl.pallas_call(
            finish_kernel,
            out_shape=[jax.ShapeDtypeStruct((rows, width), bf16)] * 2,
            in_specs=[whole()] * 2,
            out_specs=[whole()] * 2,
            compiler_params=pltpu.CompilerParams(vmem_limit_bytes=8 << 20),
            cost_estimate=pl.CostEstimate(
                flops=1_000_000, bytes_accessed=2_000_000, transcendentals=0
            ),
            name="finish",
        )(x, sums)
    )


def solution(mesh):
    fine = Mesh(mesh.devices.reshape(NX, NL, NY, NH, 2), ("x", "zl", "y", "zh", "c"))
    dp, seq = ("x", "zl"), ("y", "zh", "c")
    tokens = P(seq, dp)
    return jax.shard_map(
        on_device,
        mesh=fine,
        in_specs=(tokens,) * 9 + (P(dp + seq, None),),
        out_specs=(tokens, tokens),
        check_vma=False,
    )
```
